32 devices in a mesh: section: 4 (over y, core), dp: 8 (over z, x).
Axes of the slice: x: 2, y: 2, z: 4, core: 2. Of those that a mesh axis runs over, the one named last changes fastest.
Arguments:
- patch_tokens: bfloat16 [4, 8, 196, 1280], P(None, 'dp'), may hold values from -24 to 24
- visible: int32 [4, 8, 98], P(None, 'dp'), may hold values from 0 to 195, as said below
- keep_mask: int32 [4, 8, 98], P(None, 'dp'), may hold values from 0 to 1, as said below
- lengths: int32 [4], replicated, may hold values from 49 to 98
- qkv_weight: bfloat16 [4, 1280, 1920], P('section', 'dp'), may hold values from -4 to 4
- out_weight: bfloat16 [4, 640, 1280], P('section', 'dp'), may hold values from -0.25 to 0.25
- norm_gain: bfloat16 [4, 1280], P('section'), may hold values from 0.099609375 to 1.8984375
- targets: bfloat16 [4, 4, 8, 98, 1280], P('section', None, 'dp'), may hold values from -12 to 12
Outputs:
- hidden_states: bfloat16 [4, 4, 8, 98, 1280], P('section', None, 'dp')
- token_loss: float32 [4, 8, 98], P(None, 'dp')
- loss: float32 [4], replicated
The draws below stay inside these ranges and needn't reach their ends.
Inputs may be any that keep to these rules, and one draw needn't show every extreme that they name: `visible`: the 98 entries of one image are different patch numbers. `keep_mask`: slot 0 of every image is 1.
All inputs are finite; a program needn't handle non-finite values.
Results may differ from the reference program's by a relative error of at most 0.019.
Values may be sent and summed in bfloat16 or wider, within the bound.
A program may use at most 128 MiB of HBM per device.

```python
import jax
import jax.numpy as jnp
from jax import lax

D = 1280
HEADS = 8
HDIM = 80
NPATCH = 196
BMIN = 49
BMAX = 98
MICRO = 4
IMAGES = 8
LAYERS = 4


def draw_visible(key, part):
    row_keys = jax.random.split(key, MICRO * IMAGES)
    shuffled = jax.vmap(lambda one_key: jax.random.permutation(one_key, NPATCH))(row_keys)
    return shuffled[:, :BMAX].reshape(MICRO, IMAGES, BMAX).astype(jnp.int32)


def draw_keep_mask(key, part):
    ticket = jax.random.randint(key, (MICRO, IMAGES, BMAX), 0, 1000)
    image_pos = jnp.arange(IMAGES, dtype=jnp.int32)
    threshold = 300 + 600 * image_pos // max(IMAGES - 1, 1)
    keep_flags = (ticket < threshold[None, :, None]).astype(jnp.int32)
    leading = jnp.arange(BMAX, dtype=jnp.int32) == 0
    return jnp.where(leading[None, None, :], 1, keep_flags).astype(jnp.int32)


def patch_values(key):
    patch_key = jax.random.fold_in(key, 21)
    shape = (MICRO, IMAGES, NPATCH, D)
    values = jax.random.truncated_normal(patch_key, -6.0, 6.0, shape, jnp.float32)
    return jnp.clip(values, -24.0, 24.0).astype(jnp.bfloat16)


def draw_patch_tokens(key, part):
    return patch_values(key)


def draw_qkv_weight(key, part):
    base = jax.random.truncated_normal(key, -4.0, 4.0, (LAYERS, D, 3, HEADS, HDIM), jnp.float32) * D ** (-0.5)
    base = jnp.clip(base, -4.0, 4.0)
    return base.reshape(LAYERS, D, 3 * HEADS * HDIM).astype(jnp.bfloat16)


def draw_targets(key, part):
    shape = (LAYERS, MICRO, IMAGES, BMAX, D)
    tokens = patch_values(key)
    chosen = draw_visible(key, part)
    gathered = jnp.take_along_axis(tokens, chosen[:, :, :, None], axis=2).astype(jnp.float32)
    row_mean = jnp.mean(gathered, -1, keepdims=True)
    centered = gathered - row_mean
    variance = jnp.mean(centered * centered, -1, keepdims=True)
    base = centered * lax.rsqrt(variance + 1e-06)
    layer_pos = jnp.arange(LAYERS, dtype=jnp.float32) / max(LAYERS - 1, 1)
    image_pos = jnp.arange(IMAGES, dtype=jnp.float32) / max(IMAGES - 1, 1)
    noise_key = jax.random.fold_in(key, 31)
    noise = jax.random.truncated_normal(noise_key, -4.0, 4.0, shape, jnp.float32)
    layer_scale = 0.25 * (1.0 + 2.0 * layer_pos)
    image_scale = 1.0 + image_pos
    noise = noise * layer_scale[:, None, None, None, None] * image_scale[None, None, :, None, None]
    values = base[None] + noise
    return jnp.clip(values, -12.0, 12.0).astype(jnp.bfloat16)


def touch_ends(drawn, stream_key, least, high):
    shape = drawn.shape
    spot = [jax.random.randint(jax.random.fold_in(stream_key, axis), (), 0, shape[axis]) for axis in range(len(shape))]
    drawn = drawn.at[tuple(spot)].set(least)
    longest = shape.index(max(shape))
    spot[longest] = (spot[longest] + 1) % shape[longest]
    return drawn.at[tuple(spot)].set(high)


def level_of(stream_key, shape, cuts, least, high):
    def one(position, blocks):
        steps = jax.random.uniform(jax.random.fold_in(jax.random.fold_in(stream_key, 6), position), (blocks,), jnp.float32, least / len(cuts), high / len(cuts))
        return jnp.repeat(jnp.exp(steps), shape[position] // blocks).reshape((-1,) + (1,) * (len(shape) - position - 1))

    factor_of = one(*cuts[0])
    for cut in cuts[1:]:
        factor_of = factor_of * one(*cut)
    return factor_of


def normal_values(own_key, shape, width, most, cuts=(), held_as=jnp.bfloat16):
    drawn = jax.random.normal(own_key, shape, jnp.float32) * width
    if len(cuts) > 0:
        drawn = level_of(own_key, shape, cuts, -0.22, 0.18) * drawn
    return jnp.clip(drawn, min=-most, max=most).astype(held_as)


def setup_inputs(seed: int = 0) -> dict:
    keys = jax.random.split(jax.random.key(seed), 9)
    return {
        "patch_tokens": draw_patch_tokens(jax.random.fold_in(keys[8], 71), 0),
        "visible": draw_visible(jax.random.fold_in(keys[8], 71), 0),
        "keep_mask": draw_keep_mask(jax.random.fold_in(keys[8], 71), 0),
        "lengths": touch_ends(jax.random.randint(keys[3], (MICRO,), BMIN, BMAX + 1), jax.random.fold_in(keys[3], 1), BMIN, BMAX).astype(jnp.int32),
        "qkv_weight": draw_qkv_weight(jax.random.fold_in(keys[8], 71), 0),
        "out_weight": normal_values(keys[5], (LAYERS, HEADS * HDIM, D), (HEADS * HDIM) ** -0.5, 0.25, ((0, 4), (1, 8))),
        "norm_gain": jnp.clip(1.0 + 0.18 * jax.random.normal(keys[6], (LAYERS, D), jnp.float32), 0.099609375, 1.8984375).astype(jnp.bfloat16),
        "targets": draw_targets(jax.random.fold_in(keys[8], 71), 0),
    }


def norm_rows(values):
    row_mean = lax.optimization_barrier(jnp.mean(values, -1, keepdims=True))
    centered = values - row_mean
    variance = lax.optimization_barrier(jnp.mean(centered * centered, -1, keepdims=True))
    return centered * lax.rsqrt(variance + 1e-06)

def encoder_layer(tokens_now, live_rows, norm_scale, w_qkv, w_out):
    images, row_count, model_width = tokens_now.shape
    normed = (norm_rows(tokens_now.astype(jnp.float32)) * norm_scale).astype(jnp.bfloat16)
    projections = jnp.dot(normed.reshape(images * row_count, model_width), w_qkv, preferred_element_type=jnp.float32).astype(jnp.bfloat16)
    projections = projections.reshape(images, row_count, 3, HEADS, HDIM)
    queries = projections[:, :, 0].astype(jnp.float32)
    key_rows = projections[:, :, 1].astype(jnp.float32)
    value_rows = projections[:, :, 2].astype(jnp.float32)
    scores = jnp.einsum('iqhe,ikhe->ihqk', queries, key_rows) * HDIM ** (-0.5)
    scores = jnp.where(live_rows[:, None, None, :], scores, -1e+30)
    row_max = lax.optimization_barrier(jnp.max(scores, -1, keepdims=True))
    weights = jnp.exp(scores - row_max)
    probabilities = (weights / lax.optimization_barrier(jnp.sum(weights, -1, keepdims=True))).astype(jnp.bfloat16)
    context = jnp.einsum('ihqk,ikhe->iqhe', probabilities.astype(jnp.float32), value_rows).astype(jnp.bfloat16)
    projected = jnp.dot(context.reshape(images * row_count, HEADS * HDIM), w_out, preferred_element_type=jnp.float32)
    return (tokens_now.astype(jnp.float32) + projected.reshape(images, row_count, model_width)).astype(jnp.bfloat16)

def reference(patch_tokens, visible, keep_mask, lengths, qkv_weight, out_weight, norm_gain, targets):
    positions = jnp.arange(BMAX, dtype=jnp.int32)
    live = (positions[None, None, :] < lengths[:, None, None]) & (keep_mask == 1)
    tokens_now = jnp.take_along_axis(patch_tokens, visible[:, :, :, None], axis=2)
    tokens_now = tokens_now.reshape(MICRO * IMAGES, BMAX, D)
    flat_live = live.reshape(MICRO * IMAGES, BMAX)
    token_error = jnp.zeros((MICRO * IMAGES, BMAX), jnp.float32)
    layer_outputs = []
    for layer_index in range(LAYERS):
        tokens_now = encoder_layer(tokens_now, flat_live, norm_gain[layer_index].astype(jnp.float32), qkv_weight[layer_index], out_weight[layer_index])
        masked = jnp.where(flat_live[:, :, None], tokens_now, jnp.zeros_like(tokens_now))
        layer_outputs.append(masked.reshape(MICRO, IMAGES, BMAX, D))
        deviation = norm_rows(tokens_now.astype(jnp.float32)) - targets[layer_index].reshape(MICRO * IMAGES, BMAX, D).astype(jnp.float32)
        token_error = token_error + jnp.where(flat_live, lax.optimization_barrier(jnp.mean(deviation * deviation, -1)), jnp.float32(0.0))
    token_loss = token_error.reshape(MICRO, IMAGES, BMAX)
    count = lax.optimization_barrier(jnp.sum(live.astype(jnp.float32), axis=(1, 2)))
    loss = lax.optimization_barrier(jnp.sum(token_loss, axis=(1, 2))) / count
    return (jnp.stack(layer_outputs), token_loss, loss)
```

```python
import functools

import jax
import jax.numpy as jnp
from jax import lax
from jax.experimental import pallas as pl
from jax.experimental.pallas import tpu as pltpu
from jax.sharding import PartitionSpec as P

HEADS = 8
HDIM = 80
MESH = pl.DeviceIdType.MESH


def norm_rows(values):
    row_mean = jnp.mean(values, -1, keepdims=True)
    centered = values - row_mean
    variance = jnp.mean(centered * centered, -1, keepdims=True)
    return centered * lax.rsqrt(variance + 1e-06)


def eye_mask(rows, columns):
    shape = (rows, columns)
    return lax.broadcasted_iota(jnp.int32, shape, 0) == lax.broadcasted_iota(jnp.int32, shape, 1)


def to_column(row, rows):
    return jnp.sum(jnp.where(eye_mask(rows, row.shape[1]), row, 0.0), axis=1, keepdims=True)


def to_row(column, columns):
    return jnp.sum(jnp.where(eye_mask(column.shape[0], columns), column, 0.0), axis=0, keepdims=True)


def halves(rows):
    low = (rows // 2 + 15) // 16 * 16
    return ((0, low), (low, rows - low))


def kernel_body(
    gathers, sections, ring_size,
    lengths, patches_in, visible, keep, w_qkv_in, w_out_in, gain, targets_in,
    hidden, token_loss, loss,
    w_qkv_all, w_out_all, x_in, x_out, proj, context, keep_rows, visible_rows,
    errors, error_slots, sums, sum_slots,
    own_sem, ring_send, ring_recv, x_send, x_recv, error_send, error_recv, sum_send, sum_recv, turn_sem, targets_held, targets, targets_sem,
    patches_held, patches, patches_sem, hidden_held, hidden_sem,
):
    section = lax.axis_index("section")
    member = lax.axis_index("dp")
    micro_count, slots = targets.shape[0], targets.shape[1]
    rows = x_in.shape[1]
    width = x_in.shape[2]
    head_width = HEADS * HDIM

    pairs = ((w_qkv_in, w_qkv_all), (w_out_in, w_out_all))
    own_copies = []
    if gathers:
        for which, (shard, whole) in enumerate(pairs):
            own_rows = shard.shape[0]
            target = whole.at[pl.ds(pl.multiple_of(member * own_rows, 16), own_rows)]
            own_copies.append(pltpu.make_async_copy(shard, target, own_sem.at[which]))
            own_copies[-1].start()
    targets_copy = pltpu.make_async_copy(targets_in, targets_held, targets_sem)
    targets_copy.start()
    patches_copy = pltpu.make_async_copy(patches_in, patches_held, patches_sem)

    @pl.when(section == 0)
    def _():
        patches_copy.start()

    half = ring_size // 2
    column, line = lax.rem(member, 2), member // 2
    place = line + column * (ring_size - 1 - 2 * line)

    def device_at(position):
        position = lax.rem(position + 2 * ring_size, ring_size)
        far = position // half
        return 2 * position * (1 - far) + far * (2 * (ring_size - 1 - position) + 1)

    barrier = pltpu.get_barrier_semaphore()
    if gathers:
        greeted = [device_at(place + 1), device_at(place - 1)][:ring_size - 1]
    else:
        greeted = [lax.rem(member + distance, ring_size) for distance in range(1, ring_size)]
    for peer in greeted:
        pl.semaphore_signal(barrier, inc=1, device_id={"dp": peer}, device_id_type=MESH)
    for distance in range(1, sections):
        pl.semaphore_signal(
            barrier, inc=1, device_id={"section": lax.rem(section + distance, sections)}, device_id_type=MESH
        )
    pl.semaphore_wait(barrier, len(greeted) + sections - 1)

    def prepare():
        keep_rows[...] = jnp.zeros_like(keep_rows)
        visible_rows[...] = jnp.full(visible_rows.shape, -1.0, jnp.float32)
        keep_rows[:, :, 0:slots] = keep[...].astype(jnp.float32)
        visible_rows[:, :, 0:slots] = visible[...].astype(jnp.float32)

        targets_copy.wait()
        for m in range(micro_count):
            targets[m] = targets_held[:, m, :].astype(jnp.float32)

        @pl.when(section == 0)
        def _():
            patches_copy.wait()
            for m in range(micro_count):
                patches[m] = patches_held[:, m, :]

            def pick(m, carry):
                chosen = to_column(visible_rows[m], rows)
                patch_pos = lax.broadcasted_iota(jnp.int32, (rows, patches.shape[1]), 1).astype(jnp.float32)
                one_hot = jnp.where(patch_pos == chosen, 1.0, 0.0).astype(jnp.bfloat16)
                x_in[m] = jnp.dot(
                    one_hot, patches[m], preferred_element_type=jnp.float32
                ).astype(jnp.bfloat16)
                return carry

            lax.fori_loop(0, micro_count, pick, 0)

    if gathers:
        pieces = [(which, part) for part in (0, 1) for which in (0, 1)]

        def span(which, part, owner):
            shard_rows = pairs[which][0].shape[0]
            start, count = halves(shard_rows)[part]
            return pl.ds(pl.multiple_of(owner * shard_rows + start, 16), count)

        def hop(way, step, which, part, owner):
            there = pairs[which][1].at[span(which, part, owner)]
            index = ((way * half + step) * 2 + which) * 2 + part
            return pltpu.make_async_remote_copy(
                src_ref=there, dst_ref=there,
                send_sem=ring_send.at[index], recv_sem=ring_recv.at[index],
                device_id={"dp": device_at(place + 1 - 2 * way)}, device_id_type=MESH,
            )

        started = []

        def wanted(way, step):
            return [(w, p) for w, p in pieces if step < half - 1 or p == way]

        first = [
            hop(way, 0, w, p, member)
            for w, p in pieces for way in (0, 1) if (w, p) in wanted(way, 0)
        ]
        started.extend(first)
        early = lax.rem(section, 2) == 0
        for copy in own_copies:
            copy.wait()

        @pl.when(early)
        def _():
            for copy in first:
                copy.start()

        prepare()

        @pl.when(jnp.logical_not(early))
        def _():
            pl.semaphore_wait(turn_sem, 1)
            for copy in first:
                copy.start()

        for step in range(half):
            if step == max(half - 2, 0):
                @pl.when(early & (section + 1 < sections))
                def _():
                    pl.semaphore_signal(
                        turn_sem, inc=1, device_id={"section": lax.rem(section + 1, sections)},
                        device_id_type=MESH,
                    )

            for w, p in pieces:
                for way in (0, 1):
                    if (w, p) not in wanted(way, step):
                        continue
                    owner = device_at(place - (1 - 2 * way) * (step + 1))
                    hop(way, step, w, p, owner).wait_recv()
                    if step + 1 < half and (w, p) in wanted(way, step + 1):
                        copy = hop(way, step + 1, w, p, owner)
                        copy.start()
                        started.append(copy)
        w_qkv, w_out = w_qkv_all, w_out_all
    else:
        prepare()
        started = []
        w_qkv, w_out = w_qkv_in, w_out_in

    def pass_on(m):
        return pltpu.make_async_remote_copy(
            src_ref=x_out.at[m], dst_ref=x_in.at[m],
            send_sem=x_send.at[m], recv_sem=x_recv.at[m],
            device_id={"section": lax.rem(section + 1, sections)}, device_id_type=MESH,
        )

    def live_row(m):
        slot = lax.broadcasted_iota(jnp.int32, (1, rows), 1)
        return (keep_rows[m] > 0.5) & (slot < lengths[m])

    def layer(m, carry):
        @pl.when(section > 0)
        def _():
            pass_on(m).wait_recv()

        live = live_row(m)
        tokens = x_in[m].astype(jnp.float32)
        normed = (norm_rows(tokens) * gain[...].astype(jnp.float32)).astype(jnp.bfloat16)
        total = 3 * head_width
        for start in range(0, total, 256):
            stop = min(start + 256, total)
            proj[:, start:stop] = jnp.dot(
                normed, w_qkv[:, start:stop], preferred_element_type=jnp.float32
            ).astype(jnp.bfloat16)
        context[...] = jnp.zeros_like(context)
        for head in range(HEADS):
            low, high = head * HDIM, (head + 1) * HDIM
            left, right = low // 128 * 128, -(-high // 128) * 128
            lane = lax.broadcasted_iota(jnp.int32, (1, right - left), 1) + left
            inside = jnp.where((lane >= low) & (lane < high), 1.0, 0.0).astype(jnp.bfloat16)
            queries = proj[:, left:right] * inside
            key_rows = proj[:, head_width + left:head_width + right]
            value_rows = proj[:, 2 * head_width + left:2 * head_width + right] * inside
            scores = lax.dot_general(
                queries, key_rows, (((1,), (1,)), ((), ())), preferred_element_type=jnp.float32
            ) * HDIM ** (-0.5)
            scores = jnp.where(live, scores, -1e30)
            weights = jnp.exp(scores - jnp.max(scores, -1, keepdims=True))
            shares = (weights / jnp.sum(weights, -1, keepdims=True)).astype(jnp.bfloat16)
            context[:, left:right] += jnp.dot(shares, value_rows, preferred_element_type=jnp.float32)
        mixed = context[...].astype(jnp.bfloat16)
        for start in range(0, width, 256):
            stop = min(start + 256, width)
            x_out[m, :, start:stop] = (
                x_in[m, :, start:stop].astype(jnp.float32)
                + jnp.dot(mixed, w_out[:, start:stop], preferred_element_type=jnp.float32)
            ).astype(jnp.bfloat16)

        @pl.when(section < sections - 1)
        def _():
            pass_on(m).start()

        output = x_out[m].astype(jnp.float32)
        live_value = jnp.where(live, 1.0, 0.0)
        live_column = to_column(live_value, rows) > 0.5
        hidden_held[m] = jnp.where(live_column, output, 0.0)[0:slots].astype(jnp.bfloat16)
        pltpu.make_async_copy(hidden_held.at[m], hidden.at[m], hidden_sem.at[m]).start()
        deviation = norm_rows(output)[0:slots] - targets[m]
        error = jnp.mean(deviation * deviation, -1, keepdims=True)
        errors[m] = jnp.where(live, to_row(error, rows), 0.0)
        sums[micro_count + m] = jnp.broadcast_to(
            jnp.sum(live_value, axis=1, keepdims=True), (1, sums.shape[2])
        )
        return carry

    lax.fori_loop(0, micro_count, layer, 0)

    def error_copy(distance, slot, peer):
        return pltpu.make_async_remote_copy(
            src_ref=errors, dst_ref=error_slots.at[slot],
            send_sem=error_send.at[distance], recv_sem=error_recv.at[distance],
            device_id={"section": peer}, device_id_type=MESH,
        )

    for distance in range(1, sections):
        copy = error_copy(distance, section, lax.rem(section + distance, sections))
        copy.start()
        started.append(copy)
    error_slots[section] = errors[...]
    for distance in range(1, sections):
        sender = lax.rem(section + sections - distance, sections)
        error_copy(distance, sender, sender).wait_recv()
    error_total = error_slots[0]
    for other in range(1, sections):
        error_total = error_total + error_slots[other]
    token_loss[...] = error_total[:, :, 0:slots]
    sums[0:micro_count] = jnp.broadcast_to(
        jnp.sum(error_total, axis=2, keepdims=True), (micro_count, 1, sums.shape[2])
    )

    def sum_copy(distance, slot, peer):
        return pltpu.make_async_remote_copy(
            src_ref=sums, dst_ref=sum_slots.at[slot],
            send_sem=sum_send.at[distance], recv_sem=sum_recv.at[distance],
            device_id={"dp": peer}, device_id_type=MESH,
        )

    for distance in range(1, ring_size):
        copy = sum_copy(distance, member, lax.rem(member + distance, ring_size))
        copy.start()
        started.append(copy)
    sum_slots[member] = sums[...]
    for distance in range(1, ring_size):
        sender = lax.rem(member + ring_size - distance, ring_size)
        sum_copy(distance, sender, sender).wait_recv()
    total_sums = sum_slots[0]
    for other in range(1, ring_size):
        total_sums = total_sums + sum_slots[other]
    loss[...] = total_sums[0:micro_count] / total_sums[micro_count:2 * micro_count]

    for copy in started:
        copy.wait_send()
    for m in range(micro_count):
        pltpu.make_async_copy(hidden_held.at[m], hidden.at[m], hidden_sem.at[m]).wait()

    @pl.when(section < sections - 1)
    def _():
        for m in range(micro_count):
            pass_on(m).wait_send()


def per_device(
    patch_tokens, visible, keep_mask, lengths, qkv_weight, out_weight, norm_gain, targets
):
    sections, ring_size = lax.axis_size("section"), lax.axis_size("dp")
    micro_count, _, slots = visible.shape
    patch_count, width = patch_tokens.shape[2:]
    rows = -(-slots // 16) * 16
    w_qkv, w_out = qkv_weight[0], out_weight[0]
    gathers = ring_size % 2 == 0 and w_qkv.shape[0] % 32 == 0 and w_out.shape[0] % 16 == 0
    if not gathers:
        w_qkv = lax.all_gather(w_qkv, "dp", axis=0, tiled=True)
        w_out = lax.all_gather(w_out, "dp", axis=0, tiled=True)
    full_qkv = (width, w_qkv.shape[1]) if gathers else (16, 128)
    full_out = (HEADS * HDIM, width) if gathers else (16, 128)
    vmem = pl.BlockSpec(memory_space=pltpu.VMEM)
    hbm = pl.BlockSpec(memory_space=pltpu.HBM)
    shards = hbm if gathers else vmem
    dma = pltpu.SemaphoreType.DMA
    hidden, token_loss, loss = pl.pallas_call(
        functools.partial(kernel_body, gathers, sections, ring_size),
        out_shape=(
            jax.ShapeDtypeStruct((micro_count, slots, width), jnp.bfloat16),
            jax.ShapeDtypeStruct((micro_count, 1, slots), jnp.float32),
            jax.ShapeDtypeStruct((micro_count, 1, 128), jnp.float32),
        ),
        in_specs=[pl.BlockSpec(memory_space=pltpu.SMEM), hbm, vmem, vmem, shards, shards, vmem, hbm],
        out_specs=(hbm, vmem, vmem),
        scratch_shapes=[
            pltpu.VMEM(full_qkv, jnp.bfloat16),
            pltpu.VMEM(full_out, jnp.bfloat16),
            pltpu.VMEM((micro_count, rows, width), jnp.bfloat16),
            pltpu.VMEM((micro_count, rows, width), jnp.bfloat16),
            pltpu.VMEM((rows, 3 * HEADS * HDIM), jnp.bfloat16),
            pltpu.VMEM((rows, HEADS * HDIM), jnp.float32),
            pltpu.VMEM((micro_count, 1, rows), jnp.float32),
            pltpu.VMEM((micro_count, 1, rows), jnp.float32),
            pltpu.VMEM((micro_count, 1, rows), jnp.float32),
            pltpu.VMEM((sections, micro_count, 1, rows), jnp.float32),
            pltpu.VMEM((2 * micro_count, 1, 128), jnp.float32),
            pltpu.VMEM((ring_size, 2 * micro_count, 1, 128), jnp.float32),
            dma((2,)),
            dma((4 * ring_size,)),
            dma((4 * ring_size,)),
            dma((micro_count,)),
            dma((micro_count,)),
            dma((sections,)),
            dma((sections,)),
            dma((ring_size,)),
            dma((ring_size,)),
            pltpu.SemaphoreType.REGULAR,
            pltpu.VMEM((slots, micro_count, width), jnp.bfloat16),
            pltpu.VMEM((micro_count, slots, width), jnp.float32),
            dma,
            pltpu.VMEM((patch_count, micro_count, width), jnp.bfloat16),
            pltpu.VMEM((micro_count, patch_count, width), jnp.bfloat16),
            dma,
            pltpu.VMEM((micro_count, slots, width), jnp.bfloat16),
            dma((micro_count,)),
        ],
        compiler_params=pltpu.CompilerParams(
            collective_id=0, has_side_effects=True, vmem_limit_bytes=67043328
        ),
    )(
        lengths, jnp.transpose(patch_tokens[:, 0], (1, 0, 2)), visible, keep_mask, w_qkv, w_out, norm_gain,
        jnp.transpose(targets[0, :, 0], (1, 0, 2)),
    )
    return (hidden[None, :, None], token_loss, loss[:, 0, 0])


def solution(mesh):
    placed = (
        P(None, "dp", None, None),
        P(None, "dp", None),
        P(None, "dp", None),
        P(),
        P("section", "dp", None),
        P("section", "dp", None),
        P("section", None),
        P("section", None, "dp", None, None),
    )
    return jax.shard_map(
        per_device,
        mesh=mesh,
        in_specs=placed,
        out_specs=(P("section", None, "dp", None, None), P(None, "dp", None), P()),
        check_vma=False,
    )
```

```python
import functools

import jax
import jax.numpy as jnp
from jax import lax
from jax.experimental import pallas as pl
from jax.experimental.pallas import tpu as pltpu
from jax.sharding import PartitionSpec as P

HEADS = 8
HDIM = 80
MESH = pl.DeviceIdType.MESH


def norm_rows(values):
    row_mean = jnp.mean(values, -1, keepdims=True)
    centered = values - row_mean
    variance = jnp.mean(centered * centered, -1, keepdims=True)
    return centered * lax.rsqrt(variance + 1e-06)


def eye_mask(rows, columns):
    shape = (rows, columns)
    return lax.broadcasted_iota(jnp.int32, shape, 0) == lax.broadcasted_iota(jnp.int32, shape, 1)


def to_column(row, rows):
    return jnp.sum(jnp.where(eye_mask(rows, row.shape[1]), row, 0.0), axis=1, keepdims=True)


def to_row(column, columns):
    return jnp.sum(jnp.where(eye_mask(column.shape[0], columns), column, 0.0), axis=0, keepdims=True)


def halves(rows):
    low = (rows // 2 + 15) // 16 * 16
    return ((0, low), (low, rows - low))


def kernel_body(
    gathers, sections, ring_size,
    lengths, patches_in, visible, keep, w_qkv_in, w_out_in, gain, targets_in,
    hidden, token_loss, loss,
    w_qkv_all, w_out_all, x_in, x_out, proj, context, keep_rows, visible_rows,
    errors, error_slots, sums, sum_slots,
    own_sem, ring_send, ring_recv, x_send, x_recv, error_send, error_recv, sum_send, sum_recv, turn_sem, targets_held, targets, targets_sem,
    patches_held, patches, patches_sem, hidden_held, hidden_sem,
    w_before, mixed_all, mixed_in, x_before, before_send, before_recv, mixed_send, mixed_recv, skip_send, skip_recv,
):
    section = lax.axis_index("section")
    member = lax.axis_index("dp")
    micro_count, slots = targets.shape[0], targets.shape[1]
    rows = x_in.shape[1]
    width = x_in.shape[2]
    head_width = HEADS * HDIM

    pairs = ((w_qkv_in, w_qkv_all), (w_out_in, w_out_all), (w_out_in, w_before))
    giver = sections // 2 - 1 if gathers and sections % 2 == 0 and sections >= 4 else -2
    taker = giver + 1
    gives, takes = section == giver, section == taker
    own_copies = []
    if gathers:
        for which, (shard, whole) in enumerate(pairs[:2]):
            own_rows = shard.shape[0]
            target = whole.at[pl.ds(pl.multiple_of(member * own_rows, 16), own_rows)]
            own_copies.append(pltpu.make_async_copy(shard, target, own_sem.at[which]))
            own_copies[-1].start()
    targets_copy = pltpu.make_async_copy(targets_in, targets_held, targets_sem)
    targets_copy.start()
    patches_copy = pltpu.make_async_copy(patches_in, patches_held, patches_sem)

    @pl.when(section == 0)
    def _():
        patches_copy.start()

    half = ring_size // 2
    column, line = lax.rem(member, 2), member // 2
    place = line + column * (ring_size - 1 - 2 * line)

    def device_at(position):
        position = lax.rem(position + 2 * ring_size, ring_size)
        far = position // half
        return 2 * position * (1 - far) + far * (2 * (ring_size - 1 - position) + 1)

    barrier = pltpu.get_barrier_semaphore()
    if gathers:
        greeted = [device_at(place + 1), device_at(place - 1)][:ring_size - 1]
    else:
        greeted = [lax.rem(member + distance, ring_size) for distance in range(1, ring_size)]
    for peer in greeted:
        pl.semaphore_signal(barrier, inc=1, device_id={"dp": peer}, device_id_type=MESH)
    for distance in range(1, sections):
        pl.semaphore_signal(
            barrier, inc=1, device_id={"section": lax.rem(section + distance, sections)}, device_id_type=MESH
        )
    pl.semaphore_wait(barrier, len(greeted) + sections - 1)

    def before_copy():
        own_rows = w_out_in.shape[0]
        return pltpu.make_async_remote_copy(
            src_ref=w_out_in, dst_ref=w_before.at[pl.ds(pl.multiple_of(member * own_rows, 16), own_rows)],
            send_sem=before_send, recv_sem=before_recv,
            device_id={"section": taker}, device_id_type=MESH,
        )

    if giver >= 0:
        @pl.when(gives)
        def _():
            before_copy().start()

    def prepare():
        keep_rows[...] = jnp.zeros_like(keep_rows)
        visible_rows[...] = jnp.full(visible_rows.shape, -1.0, jnp.float32)
        keep_rows[:, :, 0:slots] = keep[...].astype(jnp.float32)
        visible_rows[:, :, 0:slots] = visible[...].astype(jnp.float32)

        targets_copy.wait()
        for m in range(micro_count):
            targets[m] = targets_held[:, m, :].astype(jnp.float32)

        @pl.when(section == 0)
        def _():
            patches_copy.wait()
            for m in range(micro_count):
                patches[m] = patches_held[:, m, :]

            def pick(m, carry):
                chosen = to_column(visible_rows[m], rows)
                patch_pos = lax.broadcasted_iota(jnp.int32, (rows, patches.shape[1]), 1).astype(jnp.float32)
                one_hot = jnp.where(patch_pos == chosen, 1.0, 0.0).astype(jnp.bfloat16)
                x_in[m] = jnp.dot(
                    one_hot, patches[m], preferred_element_type=jnp.float32
                ).astype(jnp.bfloat16)
                return carry

            lax.fori_loop(0, micro_count, pick, 0)

    if gathers:
        pieces = [(which, part) for part in (0, 1) for which in (0, 1)]

        def span(which, part, owner):
            shard_rows = pairs[which][0].shape[0]
            start, count = halves(shard_rows)[part]
            return pl.ds(pl.multiple_of(owner * shard_rows + start, 16), count)

        def hop(way, step, which, part, owner):
            there = pairs[which][1].at[span(which, part, owner)]
            index = ((way * half + step) * 3 + which) * 2 + part
            return pltpu.make_async_remote_copy(
                src_ref=there, dst_ref=there,
                send_sem=ring_send.at[index], recv_sem=ring_recv.at[index],
                device_id={"dp": device_at(place + 1 - 2 * way)}, device_id_type=MESH,
            )

        started = []

        def wanted(way, step):
            return [(w, p) for w, p in pieces if step < half - 1 or p == way]

        first = [
            hop(way, 0, w, p, member)
            for w, p in pieces for way in (0, 1) if (w, p) in wanted(way, 0)
        ]
        started.extend(first)
        early = lax.rem(section, 2) == 0
        for copy in own_copies:
            copy.wait()

        @pl.when(early)
        def _():
            for copy in first:
                copy.start()

        prepare()

        @pl.when(jnp.logical_not(early))
        def _():
            pl.semaphore_wait(turn_sem, 1)
            for copy in first:
                copy.start()

        for step in range(half):
            if step == max(half - 2, 0):
                @pl.when(early & (section + 1 < sections))
                def _():
                    pl.semaphore_signal(
                        turn_sem, inc=1, device_id={"section": lax.rem(section + 1, sections)},
                        device_id_type=MESH,
                    )

            for w, p in pieces:
                for way in (0, 1):
                    if (w, p) not in wanted(way, step):
                        continue
                    owner = device_at(place - (1 - 2 * way) * (step + 1))
                    hop(way, step, w, p, owner).wait_recv()
                    if step + 1 < half and (w, p) in wanted(way, step + 1):
                        copy = hop(way, step + 1, w, p, owner)
                        copy.start()
                        started.append(copy)
        relayed = []
        if giver >= 0:
            before = [
                hop(way, 0, 2, p, member)
                for p in (0, 1) for way in (0, 1) if (1, p) in wanted(way, 0)
            ]
            relayed.extend((0, p, way) for p in (0, 1) for way in (0, 1) if (1, p) in wanted(way, 0))

            @pl.when(takes)
            def _():
                before_copy().wait_recv()
                for copy in before:
                    copy.start()
                for step in range(half):
                    for p in (0, 1):
                        for way in (0, 1):
                            if (1, p) not in wanted(way, step):
                                continue
                            owner = device_at(place - (1 - 2 * way) * (step + 1))
                            hop(way, step, 2, p, owner).wait_recv()
                            if step + 1 < half and (1, p) in wanted(way, step + 1):
                                hop(way, step + 1, 2, p, owner).start()
                                relayed.append((step + 1, p, way))

        w_qkv, w_out = w_qkv_all, w_out_all
    else:
        relayed = []
        prepare()
        started = []
        w_qkv, w_out = w_qkv_in, w_out_in

    def pass_on(m):
        return pltpu.make_async_remote_copy(
            src_ref=x_out.at[m], dst_ref=x_in.at[m],
            send_sem=x_send.at[m], recv_sem=x_recv.at[m],
            device_id={"section": lax.rem(section + 1, sections)}, device_id_type=MESH,
        )

    def skip_copy(m):
        return pltpu.make_async_remote_copy(
            src_ref=x_out.at[m], dst_ref=x_before.at[m],
            send_sem=skip_send.at[m], recv_sem=skip_recv.at[m],
            device_id={"section": taker}, device_id_type=MESH,
        )

    def mixed_copy(m):
        return pltpu.make_async_remote_copy(
            src_ref=mixed_all.at[m], dst_ref=mixed_in.at[m],
            send_sem=mixed_send.at[m], recv_sem=mixed_recv.at[m],
            device_id={"section": taker}, device_id_type=MESH,
        )

    passes = (section < sections - 1) & jnp.logical_not(gives)

    def live_row(m):
        slot = lax.broadcasted_iota(jnp.int32, (1, rows), 1)
        return (keep_rows[m] > 0.5) & (slot < lengths[m])

    def attend(m, carry):
        @pl.when((section > 0) & jnp.logical_not(takes))
        def _():
            pass_on(m).wait_recv()

        if giver >= 0:
            @pl.when(takes)
            def _():
                skip_copy(m).wait_recv()
                mixed_copy(m).wait_recv()
                for start in range(0, width, 256):
                    stop = min(start + 256, width)
                    x_in[m, :, start:stop] = (
                        x_before[m, :, start:stop].astype(jnp.float32)
                        + jnp.dot(mixed_in[m], w_before[:, start:stop], preferred_element_type=jnp.float32)
                    ).astype(jnp.bfloat16)

        live = live_row(m)
        tokens = x_in[m].astype(jnp.float32)
        normed = (norm_rows(tokens) * gain[...].astype(jnp.float32)).astype(jnp.bfloat16)
        total = 3 * head_width
        for start in range(0, total, 256):
            stop = min(start + 256, total)
            proj[:, start:stop] = jnp.dot(
                normed, w_qkv[:, start:stop], preferred_element_type=jnp.float32
            ).astype(jnp.bfloat16)
        tiles = [(head * HDIM // 128 * 128, -(-(head + 1) * HDIM // 128) * 128) for head in range(HEADS)]
        insides, scored = [], []
        for head, (left, right) in enumerate(tiles):
            low, high = head * HDIM, (head + 1) * HDIM
            lane = lax.broadcasted_iota(jnp.int32, (1, right - left), 1) + left
            inside = jnp.where((lane >= low) & (lane < high), 1.0, 0.0).astype(jnp.bfloat16)
            insides.append(inside)
            scores = lax.dot_general(
                proj[:, left:right] * inside, proj[:, head_width + left:head_width + right],
                (((1,), (1,)), ((), ())), preferred_element_type=jnp.float32,
            ) * HDIM ** (-0.5)
            scored.append(jnp.where(live, scores, -1e30))
        peaks = [jnp.max(scores, -1, keepdims=True) for scores in scored]
        grown = [jnp.exp(scores - peak) for scores, peak in zip(scored, peaks)]
        totals = [jnp.sum(weights, -1, keepdims=True) for weights in grown]
        shares = [(weights / total).astype(jnp.bfloat16) for weights, total in zip(grown, totals)]
        columns = [None] * (head_width // 128)
        for head, (left, right) in enumerate(tiles):
            part = jnp.dot(
                shares[head], proj[:, 2 * head_width + left:2 * head_width + right] * insides[head],
                preferred_element_type=jnp.float32,
            )
            for tile in range(left // 128, right // 128):
                piece = part[:, tile * 128 - left:tile * 128 - left + 128]
                columns[tile] = piece if columns[tile] is None else columns[tile] + piece
        for tile, piece in enumerate(columns):
            mixed_all[m, :, tile * 128:tile * 128 + 128] = piece.astype(jnp.bfloat16)
        if giver >= 0:
            pl.when(gives)(mixed_copy(m).start)
        return carry

    def output(m, carry):
        mixed = mixed_all[m]
        for start in range(0, width, 256):
            stop = min(start + 256, width)
            x_out[m, :, start:stop] = (
                x_in[m, :, start:stop].astype(jnp.float32)
                + jnp.dot(mixed, w_out[:, start:stop], preferred_element_type=jnp.float32)
            ).astype(jnp.bfloat16)

        pl.when(passes)(pass_on(m).start)
        if giver > 0:
            pl.when(section == giver - 1)(skip_copy(m).start)
        return carry

    def report(m, carry):
        live = live_row(m)
        output = x_out[m].astype(jnp.float32)
        live_value = jnp.where(live, 1.0, 0.0)
        live_column = to_column(live_value, rows) > 0.5
        hidden_held[m] = jnp.where(live_column, output, 0.0)[0:slots].astype(jnp.bfloat16)
        pltpu.make_async_copy(hidden_held.at[m], hidden.at[m], hidden_sem.at[m]).start()
        deviation = norm_rows(output)[0:slots] - targets[m]
        error = jnp.mean(deviation * deviation, -1, keepdims=True)
        errors[m] = jnp.where(live, to_row(error, rows), 0.0)
        sums[micro_count + m] = jnp.broadcast_to(
            jnp.sum(live_value, axis=1, keepdims=True), (1, sums.shape[2])
        )
        return carry

    def both(m, carry):
        return output(m, attend(m, carry))

    @pl.when(gives)
    def _():
        lax.fori_loop(0, micro_count, attend, 0)
        lax.fori_loop(0, micro_count, output, 0)
        lax.fori_loop(0, micro_count, report, 0)

    @pl.when(section == sections - 1)
    def _():
        lax.fori_loop(0, micro_count, lambda m, carry: report(m, both(m, carry)), 0)

    @pl.when((section < sections - 1) & jnp.logical_not(gives))
    def _():
        lax.fori_loop(0, micro_count, both, 0)
        lax.fori_loop(0, micro_count, report, 0)

    def error_copy(distance, slot, peer):
        return pltpu.make_async_remote_copy(
            src_ref=errors, dst_ref=error_slots.at[slot],
            send_sem=error_send.at[distance], recv_sem=error_recv.at[distance],
            device_id={"section": peer}, device_id_type=MESH,
        )

    for distance in range(1, sections):
        copy = error_copy(distance, section, lax.rem(section + distance, sections))
        copy.start()
        started.append(copy)
    error_slots[section] = errors[...]
    for distance in range(1, sections):
        sender = lax.rem(section + sections - distance, sections)
        error_copy(distance, sender, sender).wait_recv()
    error_total = error_slots[0]
    for other in range(1, sections):
        error_total = error_total + error_slots[other]
    token_loss[...] = error_total[:, :, 0:slots]
    sums[0:micro_count] = jnp.broadcast_to(
        jnp.sum(error_total, axis=2, keepdims=True), (micro_count, 1, sums.shape[2])
    )

    def sum_copy(distance, slot, peer):
        return pltpu.make_async_remote_copy(
            src_ref=sums, dst_ref=sum_slots.at[slot],
            send_sem=sum_send.at[distance], recv_sem=sum_recv.at[distance],
            device_id={"dp": peer}, device_id_type=MESH,
        )

    for distance in range(1, ring_size):
        copy = sum_copy(distance, member, lax.rem(member + distance, ring_size))
        copy.start()
        started.append(copy)
    sum_slots[member] = sums[...]
    for distance in range(1, ring_size):
        sender = lax.rem(member + ring_size - distance, ring_size)
        sum_copy(distance, sender, sender).wait_recv()
    total_sums = sum_slots[0]
    for other in range(1, ring_size):
        total_sums = total_sums + sum_slots[other]
    loss[...] = total_sums[0:micro_count] / total_sums[micro_count:2 * micro_count]

    for copy in started:
        copy.wait_send()
    for m in range(micro_count):
        pltpu.make_async_copy(hidden_held.at[m], hidden.at[m], hidden_sem.at[m]).wait()

    @pl.when(passes)
    def _():
        for m in range(micro_count):
            pass_on(m).wait_send()

    if giver >= 0:
        @pl.when(takes)
        def _():
            for step, p, way in relayed:
                hop(way, step, 2, p, device_at(place - (1 - 2 * way) * step)).wait_send()

        @pl.when(gives)
        def _():
            before_copy().wait_send()
            for m in range(micro_count):
                mixed_copy(m).wait_send()

        @pl.when(section == giver - 1)
        def _():
            for m in range(micro_count):
                skip_copy(m).wait_send()


def per_device(
    patch_tokens, visible, keep_mask, lengths, qkv_weight, out_weight, norm_gain, targets
):
    sections, ring_size = lax.axis_size("section"), lax.axis_size("dp")
    micro_count, _, slots = visible.shape
    patch_count, width = patch_tokens.shape[2:]
    rows = slots
    w_qkv, w_out = qkv_weight[0], out_weight[0]
    gathers = ring_size % 2 == 0 and w_qkv.shape[0] % 32 == 0 and w_out.shape[0] % 16 == 0
    if not gathers:
        w_qkv = lax.all_gather(w_qkv, "dp", axis=0, tiled=True)
        w_out = lax.all_gather(w_out, "dp", axis=0, tiled=True)
    full_qkv = (width, w_qkv.shape[1]) if gathers else (16, 128)
    full_out = (HEADS * HDIM, width) if gathers else (16, 128)
    vmem = pl.BlockSpec(memory_space=pltpu.VMEM)
    hbm = pl.BlockSpec(memory_space=pltpu.HBM)
    shards = hbm if gathers else vmem
    dma = pltpu.SemaphoreType.DMA
    hidden, token_loss, loss = pl.pallas_call(
        functools.partial(kernel_body, gathers, sections, ring_size),
        out_shape=(
            jax.ShapeDtypeStruct((micro_count, slots, width), jnp.bfloat16),
            jax.ShapeDtypeStruct((micro_count, 1, slots), jnp.float32),
            jax.ShapeDtypeStruct((micro_count, 1, 128), jnp.float32),
        ),
        in_specs=[pl.BlockSpec(memory_space=pltpu.SMEM), hbm, vmem, vmem, shards, shards, vmem, hbm],
        out_specs=(hbm, vmem, vmem),
        scratch_shapes=[
            pltpu.VMEM(full_qkv, jnp.bfloat16),
            pltpu.VMEM(full_out, jnp.bfloat16),
            pltpu.VMEM((micro_count, rows, width), jnp.bfloat16),
            pltpu.VMEM((micro_count, rows, width), jnp.bfloat16),
            pltpu.VMEM((rows, 3 * HEADS * HDIM), jnp.bfloat16),
            pltpu.VMEM((rows, HEADS * HDIM), jnp.float32),
            pltpu.VMEM((micro_count, 1, rows), jnp.float32),
            pltpu.VMEM((micro_count, 1, rows), jnp.float32),
            pltpu.VMEM((micro_count, 1, rows), jnp.float32),
            pltpu.VMEM((sections, micro_count, 1, rows), jnp.float32),
            pltpu.VMEM((2 * micro_count, 1, 128), jnp.float32),
            pltpu.VMEM((ring_size, 2 * micro_count, 1, 128), jnp.float32),
            dma((2,)),
            dma((6 * ring_size,)),
            dma((6 * ring_size,)),
            dma((micro_count,)),
            dma((micro_count,)),
            dma((sections,)),
            dma((sections,)),
            dma((ring_size,)),
            dma((ring_size,)),
            pltpu.SemaphoreType.REGULAR,
            pltpu.VMEM((slots, micro_count, width), jnp.bfloat16),
            pltpu.VMEM((micro_count, slots, width), jnp.float32),
            dma,
            pltpu.VMEM((patch_count, micro_count, width), jnp.bfloat16),
            pltpu.VMEM((micro_count, patch_count, width), jnp.bfloat16),
            dma,
            pltpu.VMEM((micro_count, slots, width), jnp.bfloat16),
            dma((micro_count,)),
            pltpu.VMEM(full_out, jnp.bfloat16),
            pltpu.VMEM((micro_count, rows, HEADS * HDIM), jnp.bfloat16),
            pltpu.VMEM((micro_count, rows, HEADS * HDIM), jnp.bfloat16),
            pltpu.VMEM((micro_count, rows, width), jnp.bfloat16),
            dma,
            dma,
            dma((micro_count,)),
            dma((micro_count,)),
            dma((micro_count,)),
            dma((micro_count,)),
        ],
        compiler_params=pltpu.CompilerParams(
            collective_id=0, has_side_effects=True, vmem_limit_bytes=67043328
        ),
    )(
        lengths, jnp.transpose(patch_tokens[:, 0], (1, 0, 2)), visible, keep_mask, w_qkv, w_out, norm_gain,
        jnp.transpose(targets[0, :, 0], (1, 0, 2)),
    )
    return (hidden[None, :, None], token_loss, loss[:, 0, 0])


def solution(mesh):
    placed = (
        P(None, "dp", None, None),
        P(None, "dp", None),
        P(None, "dp", None),
        P(),
        P("section", "dp", None),
        P("section", "dp", None),
        P("section", None),
        P("section", None, "dp", None, None),
    )
    return jax.shard_map(
        per_device,
        mesh=mesh,
        in_specs=placed,
        out_specs=(P("section", None, "dp", None, None), P(None, "dp", None), P()),
        check_vma=False,
    )
```

```python
import functools

import jax
import jax.numpy as jnp
from jax import lax
from jax.experimental import pallas as pl
from jax.experimental.pallas import tpu as pltpu
from jax.sharding import PartitionSpec as P

HEADS = 8
HDIM = 80
MESH = pl.DeviceIdType.MESH


def norm_rows(values):
    row_mean = jnp.mean(values, -1, keepdims=True)
    centered = values - row_mean
    variance = jnp.mean(centered * centered, -1, keepdims=True)
    return centered * lax.rsqrt(variance + 1e-06)


def eye_mask(rows, columns):
    shape = (rows, columns)
    return lax.broadcasted_iota(jnp.int32, shape, 0) == lax.broadcasted_iota(jnp.int32, shape, 1)


def to_column(row, rows):
    return jnp.sum(jnp.where(eye_mask(rows, row.shape[1]), row, 0.0), axis=1, keepdims=True)


def to_row(column, columns):
    return jnp.sum(jnp.where(eye_mask(column.shape[0], columns), column, 0.0), axis=0, keepdims=True)


def halves(rows):
    low = (rows // 2 + 15) // 16 * 16
    return ((0, low), (low, rows - low))


def kernel_body(
    gathers, sections, ring_size,
    lengths, patches_in, visible, keep, w_qkv_in, w_out_in, gain, targets_in,
    hidden, token_loss, loss,
    w_qkv_all, w_out_all, x_in, x_out, proj, context, keep_rows, visible_rows,
    errors, error_slots, sums, sum_slots,
    own_sem, ring_send, ring_recv, x_send, x_recv, error_send, error_recv, sum_send, sum_recv, turn_sem, targets_held, targets, targets_sem,
    patches_held, patches, patches_sem, hidden_held, hidden_sem,
    w_before, mixed_all, mixed_in, x_before, before_send, before_recv, mixed_send, mixed_recv, skip_send, skip_recv,
):
    section = lax.axis_index("section")
    member = lax.axis_index("dp")
    micro_count, slots = targets.shape[0], targets.shape[1]
    rows = x_in.shape[1]
    width = x_in.shape[2]
    head_width = HEADS * HDIM

    pairs = ((w_qkv_in, w_qkv_all), (w_out_in, w_out_all))
    giver = sections // 2 - 1 if gathers and sections % 2 == 0 and sections >= 4 else -2
    taker = giver + 1
    gives, takes = section == giver, section == taker
    own_copies = []
    if gathers:
        for which, (shard, whole) in enumerate(pairs):
            own_rows = shard.shape[0]
            target = whole.at[pl.ds(pl.multiple_of(member * own_rows, 16), own_rows)]
            own_copies.append(pltpu.make_async_copy(shard, target, own_sem.at[which]))
            own_copies[-1].start()
    targets_copy = pltpu.make_async_copy(targets_in, targets_held, targets_sem)
    targets_copy.start()
    patches_copy = pltpu.make_async_copy(patches_in, patches_held, patches_sem)

    @pl.when(section == 0)
    def _():
        patches_copy.start()

    half = ring_size // 2
    column, line = lax.rem(member, 2), member // 2
    place = line + column * (ring_size - 1 - 2 * line)

    def device_at(position):
        position = lax.rem(position + 2 * ring_size, ring_size)
        far = position // half
        return 2 * position * (1 - far) + far * (2 * (ring_size - 1 - position) + 1)

    barrier = pltpu.get_barrier_semaphore()
    if gathers:
        greeted = [device_at(place + 1), device_at(place - 1)][:ring_size - 1]
    else:
        greeted = [lax.rem(member + distance, ring_size) for distance in range(1, ring_size)]
    for peer in greeted:
        pl.semaphore_signal(barrier, inc=1, device_id={"dp": peer}, device_id_type=MESH)
    for distance in range(1, sections):
        pl.semaphore_signal(
            barrier, inc=1, device_id={"section": lax.rem(section + distance, sections)}, device_id_type=MESH
        )
    pl.semaphore_wait(barrier, len(greeted) + sections - 1)

    def before_copy():
        own_rows = w_out_in.shape[0]
        return pltpu.make_async_remote_copy(
            src_ref=w_out_in, dst_ref=w_before.at[pl.ds(pl.multiple_of(member * own_rows, 16), own_rows)],
            send_sem=before_send, recv_sem=before_recv,
            device_id={"section": taker}, device_id_type=MESH,
        )

    def share_copy(there):
        return pltpu.make_async_remote_copy(
            src_ref=w_out_all.at[there], dst_ref=w_before.at[there],
            send_sem=before_send, recv_sem=before_recv,
            device_id={"section": taker}, device_id_type=MESH,
        )

    if giver >= 0:
        @pl.when(gives)
        def _():
            before_copy().start()

    def prepare():
        keep_rows[...] = jnp.zeros_like(keep_rows)
        visible_rows[...] = jnp.full(visible_rows.shape, -1.0, jnp.float32)
        keep_rows[:, :, 0:slots] = keep[...].astype(jnp.float32)
        visible_rows[:, :, 0:slots] = visible[...].astype(jnp.float32)

        targets_copy.wait()
        for m in range(micro_count):
            targets[m] = targets_held[:, m, :].astype(jnp.float32)

        @pl.when(section == 0)
        def _():
            patches_copy.wait()
            for m in range(micro_count):
                patches[m] = patches_held[:, m, :]

            def pick(m, carry):
                chosen = to_column(visible_rows[m], rows)
                patch_pos = lax.broadcasted_iota(jnp.int32, (rows, patches.shape[1]), 1).astype(jnp.float32)
                one_hot = jnp.where(patch_pos == chosen, 1.0, 0.0).astype(jnp.bfloat16)
                x_in[m] = jnp.dot(
                    one_hot, patches[m], preferred_element_type=jnp.float32
                ).astype(jnp.bfloat16)
                return carry

            lax.fori_loop(0, micro_count, pick, 0)

    if gathers:
        pieces = [(which, part) for which in (1, 0) for part in (0, 1)]

        def span(which, part, owner):
            shard_rows = pairs[which][0].shape[0]
            start, count = halves(shard_rows)[part]
            return pl.ds(pl.multiple_of(owner * shard_rows + start, 16), count)

        def hop(way, step, which, part, owner):
            there = pairs[which][1].at[span(which, part, owner)]
            index = ((way * half + step) * 2 + which) * 2 + part
            return pltpu.make_async_remote_copy(
                src_ref=there, dst_ref=there,
                send_sem=ring_send.at[index], recv_sem=ring_recv.at[index],
                device_id={"dp": device_at(place + 1 - 2 * way)}, device_id_type=MESH,
            )

        started = []

        def wanted(way, step):
            return [(w, p) for w, p in pieces if step < half - 1 or p == way]

        first = [
            hop(way, 0, w, p, member)
            for w, p in pieces for way in (0, 1) if (w, p) in wanted(way, 0)
        ]
        started.extend(first)
        early = lax.rem(section, 2) == 0
        for copy in own_copies:
            copy.wait()

        @pl.when(early)
        def _():
            for copy in first:
                copy.start()

        prepare()

        @pl.when(jnp.logical_not(early))
        def _():
            pl.semaphore_wait(turn_sem, 1)
            for copy in first:
                copy.start()

        for step in range(half):
            if step == max(half - 2, 0):
                @pl.when(early & (section + 1 < sections))
                def _():
                    pl.semaphore_signal(
                        turn_sem, inc=1, device_id={"section": lax.rem(section + 1, sections)},
                        device_id_type=MESH,
                    )

            for w, p in pieces:
                for way in (0, 1):
                    if (w, p) not in wanted(way, step):
                        continue
                    owner = device_at(place - (1 - 2 * way) * (step + 1))
                    hop(way, step, w, p, owner).wait_recv()
                    if step + 1 < half and (w, p) in wanted(way, step + 1):
                        copy = hop(way, step + 1, w, p, owner)
                        copy.start()
                        started.append(copy)
                    if w == 1 and giver >= 0:
                        pl.when(gives)(share_copy(span(1, p, owner)).start)
        w_qkv, w_out = w_qkv_all, w_out_all
    else:
        prepare()
        started = []
        w_qkv, w_out = w_qkv_in, w_out_in

    def pass_on(m):
        return pltpu.make_async_remote_copy(
            src_ref=x_out.at[m], dst_ref=x_in.at[m],
            send_sem=x_send.at[m], recv_sem=x_recv.at[m],
            device_id={"section": lax.rem(section + 1, sections)}, device_id_type=MESH,
        )

    def skip_copy(m):
        return pltpu.make_async_remote_copy(
            src_ref=x_out.at[m], dst_ref=x_before.at[m],
            send_sem=skip_send.at[m], recv_sem=skip_recv.at[m],
            device_id={"section": taker}, device_id_type=MESH,
        )

    def mixed_copy(m):
        return pltpu.make_async_remote_copy(
            src_ref=mixed_all.at[m], dst_ref=mixed_in.at[m],
            send_sem=mixed_send.at[m], recv_sem=mixed_recv.at[m],
            device_id={"section": taker}, device_id_type=MESH,
        )

    passes = (section < sections - 1) & jnp.logical_not(gives)

    def live_row(m):
        slot = lax.broadcasted_iota(jnp.int32, (1, rows), 1)
        return (keep_rows[m] > 0.5) & (slot < lengths[m])

    def attend(m, carry):
        @pl.when((section > 0) & jnp.logical_not(takes))
        def _():
            pass_on(m).wait_recv()

        if giver >= 0:
            @pl.when(takes)
            def _():
                skip_copy(m).wait_recv()
                mixed_copy(m).wait_recv()
                for start in range(0, width, 256):
                    stop = min(start + 256, width)
                    x_in[m, :, start:stop] = (
                        x_before[m, :, start:stop].astype(jnp.float32)
                        + jnp.dot(mixed_in[m], w_before[:, start:stop], preferred_element_type=jnp.float32)
                    ).astype(jnp.bfloat16)

        live = live_row(m)
        tokens = x_in[m].astype(jnp.float32)
        normed = (norm_rows(tokens) * gain[...].astype(jnp.float32)).astype(jnp.bfloat16)
        total = 3 * head_width
        for start in range(0, total, 256):
            stop = min(start + 256, total)
            proj[:, start:stop] = jnp.dot(
                normed, w_qkv[:, start:stop], preferred_element_type=jnp.float32
            ).astype(jnp.bfloat16)
        tiles = [(head * HDIM // 128 * 128, -(-(head + 1) * HDIM // 128) * 128) for head in range(HEADS)]
        insides, scored = [], []
        for head, (left, right) in enumerate(tiles):
            low, high = head * HDIM, (head + 1) * HDIM
            lane = lax.broadcasted_iota(jnp.int32, (1, right - left), 1) + left
            inside = jnp.where((lane >= low) & (lane < high), 1.0, 0.0).astype(jnp.bfloat16)
            insides.append(inside)
            scores = lax.dot_general(
                proj[:, left:right] * inside, proj[:, head_width + left:head_width + right],
                (((1,), (1,)), ((), ())), preferred_element_type=jnp.float32,
            ) * HDIM ** (-0.5)
            scored.append(jnp.where(live, scores, -1e30))
        peaks = [jnp.max(scores, -1, keepdims=True) for scores in scored]
        grown = [jnp.exp(scores - peak) for scores, peak in zip(scored, peaks)]
        totals = [jnp.sum(weights, -1, keepdims=True) for weights in grown]
        shares = [(weights / total).astype(jnp.bfloat16) for weights, total in zip(grown, totals)]
        columns = [None] * (head_width // 128)
        for head, (left, right) in enumerate(tiles):
            part = jnp.dot(
                shares[head], proj[:, 2 * head_width + left:2 * head_width + right] * insides[head],
                preferred_element_type=jnp.float32,
            )
            for tile in range(left // 128, right // 128):
                piece = part[:, tile * 128 - left:tile * 128 - left + 128]
                columns[tile] = piece if columns[tile] is None else columns[tile] + piece
        for tile, piece in enumerate(columns):
            mixed_all[m, :, tile * 128:tile * 128 + 128] = piece.astype(jnp.bfloat16)
        if giver >= 0:
            pl.when(gives)(mixed_copy(m).start)
        return carry

    def output(m, carry):
        mixed = mixed_all[m]
        for start in range(0, width, 256):
            stop = min(start + 256, width)
            x_out[m, :, start:stop] = (
                x_in[m, :, start:stop].astype(jnp.float32)
                + jnp.dot(mixed, w_out[:, start:stop], preferred_element_type=jnp.float32)
            ).astype(jnp.bfloat16)

        pl.when(passes)(pass_on(m).start)
        if giver > 0:
            pl.when(section == giver - 1)(skip_copy(m).start)
        return carry

    def report(m, carry):
        live = live_row(m)
        output = x_out[m].astype(jnp.float32)
        live_value = jnp.where(live, 1.0, 0.0)
        live_column = to_column(live_value, rows) > 0.5
        hidden_held[m] = jnp.where(live_column, output, 0.0)[0:slots].astype(jnp.bfloat16)
        pltpu.make_async_copy(hidden_held.at[m], hidden.at[m], hidden_sem.at[m]).start()
        deviation = norm_rows(output)[0:slots] - targets[m]
        error = jnp.mean(deviation * deviation, -1, keepdims=True)
        errors[m] = jnp.where(live, to_row(error, rows), 0.0)
        sums[micro_count + m] = jnp.broadcast_to(
            jnp.sum(live_value, axis=1, keepdims=True), (1, sums.shape[2])
        )
        return carry

    def both(m, carry):
        return output(m, attend(m, carry))

    if giver >= 0:
        @pl.when(takes)
        def _():
            share_copy(pl.ds(0, w_before.shape[0])).wait_recv()

    @pl.when(gives)
    def _():
        lax.fori_loop(0, micro_count, attend, 0)
        lax.fori_loop(0, micro_count, output, 0)
        lax.fori_loop(0, micro_count, report, 0)

    @pl.when(section == sections - 1)
    def _():
        lax.fori_loop(0, micro_count, lambda m, carry: report(m, both(m, carry)), 0)

    @pl.when((section < sections - 1) & jnp.logical_not(gives))
    def _():
        lax.fori_loop(0, micro_count, both, 0)
        lax.fori_loop(0, micro_count, report, 0)

    def error_copy(distance, slot, peer):
        return pltpu.make_async_remote_copy(
            src_ref=errors, dst_ref=error_slots.at[slot],
            send_sem=error_send.at[distance], recv_sem=error_recv.at[distance],
            device_id={"section": peer}, device_id_type=MESH,
        )

    for distance in range(1, sections):
        copy = error_copy(distance, section, lax.rem(section + distance, sections))
        copy.start()
        started.append(copy)
    error_slots[section] = errors[...]
    for distance in range(1, sections):
        sender = lax.rem(section + sections - distance, sections)
        error_copy(distance, sender, sender).wait_recv()
    error_total = error_slots[0]
    for other in range(1, sections):
        error_total = error_total + error_slots[other]
    token_loss[...] = error_total[:, :, 0:slots]
    sums[0:micro_count] = jnp.broadcast_to(
        jnp.sum(error_total, axis=2, keepdims=True), (micro_count, 1, sums.shape[2])
    )

    def sum_copy(distance, slot, peer):
        return pltpu.make_async_remote_copy(
            src_ref=sums, dst_ref=sum_slots.at[slot],
            send_sem=sum_send.at[distance], recv_sem=sum_recv.at[distance],
            device_id={"dp": peer}, device_id_type=MESH,
        )

    for distance in range(1, ring_size):
        copy = sum_copy(distance, member, lax.rem(member + distance, ring_size))
        copy.start()
        started.append(copy)
    sum_slots[member] = sums[...]
    for distance in range(1, ring_size):
        sender = lax.rem(member + ring_size - distance, ring_size)
        sum_copy(distance, sender, sender).wait_recv()
    total_sums = sum_slots[0]
    for other in range(1, ring_size):
        total_sums = total_sums + sum_slots[other]
    loss[...] = total_sums[0:micro_count] / total_sums[micro_count:2 * micro_count]

    for copy in started:
        copy.wait_send()
    for m in range(micro_count):
        pltpu.make_async_copy(hidden_held.at[m], hidden.at[m], hidden_sem.at[m]).wait()

    @pl.when(passes)
    def _():
        for m in range(micro_count):
            pass_on(m).wait_send()

    if giver >= 0:
        @pl.when(gives)
        def _():
            share_copy(pl.ds(0, w_before.shape[0])).wait_send()
            for m in range(micro_count):
                mixed_copy(m).wait_send()

        @pl.when(section == giver - 1)
        def _():
            for m in range(micro_count):
                skip_copy(m).wait_send()


def per_device(
    patch_tokens, visible, keep_mask, lengths, qkv_weight, out_weight, norm_gain, targets
):
    sections, ring_size = lax.axis_size("section"), lax.axis_size("dp")
    micro_count, _, slots = visible.shape
    patch_count, width = patch_tokens.shape[2:]
    rows = slots
    w_qkv, w_out = qkv_weight[0], out_weight[0]
    gathers = ring_size % 2 == 0 and w_qkv.shape[0] % 32 == 0 and w_out.shape[0] % 16 == 0
    if not gathers:
        w_qkv = lax.all_gather(w_qkv, "dp", axis=0, tiled=True)
        w_out = lax.all_gather(w_out, "dp", axis=0, tiled=True)
    full_qkv = (width, w_qkv.shape[1]) if gathers else (16, 128)
    full_out = (HEADS * HDIM, width) if gathers else (16, 128)
    vmem = pl.BlockSpec(memory_space=pltpu.VMEM)
    hbm = pl.BlockSpec(memory_space=pltpu.HBM)
    shards = hbm if gathers else vmem
    dma = pltpu.SemaphoreType.DMA
    hidden, token_loss, loss = pl.pallas_call(
        functools.partial(kernel_body, gathers, sections, ring_size),
        out_shape=(
            jax.ShapeDtypeStruct((micro_count, slots, width), jnp.bfloat16),
            jax.ShapeDtypeStruct((micro_count, 1, slots), jnp.float32),
            jax.ShapeDtypeStruct((micro_count, 1, 128), jnp.float32),
        ),
        in_specs=[pl.BlockSpec(memory_space=pltpu.SMEM), hbm, vmem, vmem, shards, shards, vmem, hbm],
        out_specs=(hbm, vmem, vmem),
        scratch_shapes=[
            pltpu.VMEM(full_qkv, jnp.bfloat16),
            pltpu.VMEM(full_out, jnp.bfloat16),
            pltpu.VMEM((micro_count, rows, width), jnp.bfloat16),
            pltpu.VMEM((micro_count, rows, width), jnp.bfloat16),
            pltpu.VMEM((rows, 3 * HEADS * HDIM), jnp.bfloat16),
            pltpu.VMEM((rows, HEADS * HDIM), jnp.float32),
            pltpu.VMEM((micro_count, 1, rows), jnp.float32),
            pltpu.VMEM((micro_count, 1, rows), jnp.float32),
            pltpu.VMEM((micro_count, 1, rows), jnp.float32),
            pltpu.VMEM((sections, micro_count, 1, rows), jnp.float32),
            pltpu.VMEM((2 * micro_count, 1, 128), jnp.float32),
            pltpu.VMEM((ring_size, 2 * micro_count, 1, 128), jnp.float32),
            dma((2,)),
            dma((4 * ring_size,)),
            dma((4 * ring_size,)),
            dma((micro_count,)),
            dma((micro_count,)),
            dma((sections,)),
            dma((sections,)),
            dma((ring_size,)),
            dma((ring_size,)),
            pltpu.SemaphoreType.REGULAR,
            pltpu.VMEM((slots, micro_count, width), jnp.bfloat16),
            pltpu.VMEM((micro_count, slots, width), jnp.float32),
            dma,
            pltpu.VMEM((patch_count, micro_count, width), jnp.bfloat16),
            pltpu.VMEM((micro_count, patch_count, width), jnp.bfloat16),
            dma,
            pltpu.VMEM((micro_count, slots, width), jnp.bfloat16),
            dma((micro_count,)),
            pltpu.VMEM(full_out, jnp.bfloat16),
            pltpu.VMEM((micro_count, rows, HEADS * HDIM), jnp.bfloat16),
            pltpu.VMEM((micro_count, rows, HEADS * HDIM), jnp.bfloat16),
            pltpu.VMEM((micro_count, rows, width), jnp.bfloat16),
            dma,
            dma,
            dma((micro_count,)),
            dma((micro_count,)),
            dma((micro_count,)),
            dma((micro_count,)),
        ],
        compiler_params=pltpu.CompilerParams(
            collective_id=0, has_side_effects=True, vmem_limit_bytes=67043328
        ),
    )(
        lengths, jnp.transpose(patch_tokens[:, 0], (1, 0, 2)), visible, keep_mask, w_qkv, w_out, norm_gain,
        jnp.transpose(targets[0, :, 0], (1, 0, 2)),
    )
    return (hidden[None, :, None], token_loss, loss[:, 0, 0])


def solution(mesh):
    placed = (
        P(None, "dp", None, None),
        P(None, "dp", None),
        P(None, "dp", None),
        P(),
        P("section", "dp", None),
        P("section", "dp", None),
        P("section", None),
        P("section", None, "dp", None, None),
    )
    return jax.shard_map(
        per_device,
        mesh=mesh,
        in_specs=placed,
        out_specs=(P("section", None, "dp", None, None), P(None, "dp", None), P()),
        check_vma=False,
    )
```
